32 devices in a mesh: tp: 8 (over z, y), kv: 4 (over x, core).
Axes of the slice: x: 2, y: 2, z: 4, core: 2. Of those that a mesh axis runs over, the one named last changes fastest.
Arguments:
- hidden_in: bfloat16 [2048, 4096], P(('kv', 'tp')), may hold values from -6 to 6
- gain_attn: float32 [4096], replicated, may hold values from 0.4 to 1.6
- w_qkv: bfloat16 [4096, 32, 384], P(None, 'tp'), may hold values from -0.09375 to 0.09375
- cache_kv: bfloat16 [2, 8192, 32, 256], P(None, 'kv', 'tp'), may hold values from -110 to 110
- cache_len: int32 [2], replicated, may hold values from 128 to 8192, as said below
- w_out: bfloat16 [4096, 4096], P('tp'), may hold values from -0.1875 to 0.1875
- gain_mlp: float32 [4096], replicated, may hold values from 0.1 to 1.9
- w_gate_up: bfloat16 [4096, 2, 11008], P('kv', None, 'tp'), may hold values from -0.09375 to 0.09375
- w_down: bfloat16 [11008, 4096], P('tp', 'kv'), may hold values from -0.0546875 to 0.0546875
Outputs:
- layer_out: bfloat16 [2048, 4096], P(('kv', 'tp'))
The draws below stay inside these ranges and needn't reach their ends.
Inputs may be any that keep to these rules, and one draw needn't show every extreme that they name: `cache_len`: every length is a multiple of 128; some sequence uses the whole cache.
All inputs are finite; a program needn't handle non-finite values.
Results may differ from the reference program's by a relative error of at most 0.019.
The reference program's roundings to bfloat16 on the way count: a program that leaves them out, or rounds other values in their place, can miss the bound.
Values may be sent and summed in bfloat16 or wider, within the bound.
A program may use at most 192 MiB of HBM per device.

```python
import math
import jax
import jax.numpy as jnp
from jax import lax

D = 4096
HEADS = 32
HEAD_SIZE = 128
FF = 11008
SPAN = 1024
CACHE = 8192
BATCH = 2
TOKENS = 2048


def draw_cache_kv(key, part):
    shape = (BATCH, CACHE, HEADS, 2 * HEAD_SIZE)
    return jnp.clip(jax.random.normal(key, shape, jnp.float32), -6.0, 6.0).astype(jnp.bfloat16)


def draw_cache_len(key, part):
    blocks = CACHE // 128
    order = jax.random.permutation(key, blocks)
    picked = order[jnp.arange(BATCH) % blocks]
    full_seq = jax.random.randint(jax.random.fold_in(key, 7), (), 0, BATCH)
    picked = jnp.where(jnp.arange(BATCH) == full_seq, blocks - 1, picked)
    return ((picked + 1) * 128).astype(jnp.int32)


def block_scale(own_key, dims, shards, smallest, high):
    def one(axis_at, parts):
        draws = jax.random.uniform(jax.random.fold_in(jax.random.fold_in(own_key, 6), axis_at), (parts,), jnp.float32, smallest / len(shards), high / len(shards))
        return jnp.repeat(jnp.exp(draws), dims[axis_at] // parts).reshape((-1,) + (1,) * (len(dims) - axis_at - 1))

    gain = one(*shards[0])
    for cut in shards[1:]:
        gain = gain * one(*cut)
    return gain


def centred(key, shape, spread, reach, cuts=(), kind=jnp.bfloat16):
    drawn = jax.random.normal(key, shape, jnp.float32) * spread
    if len(cuts) > 0:
        drawn = block_scale(key, shape, cuts, -0.22, 0.18) * drawn
    return jnp.clip(drawn, min=-reach, max=reach).astype(kind)


def setup_inputs(seed: int = 0) -> dict:
    key_list = jax.random.split(jax.random.key(seed), 10)
    hidden_in = centred(key_list[0], (TOKENS, D), 1.0, 6.0, ((0, 32),))
    gain_attn = jnp.clip(jax.random.uniform(key_list[1], (D,), jnp.float32, 0.4, 1.6), 0.4, 1.6)
    w_qkv = centred(key_list[2], (D, HEADS, 3 * HEAD_SIZE), D ** -0.5, 0.09375, ((1, 8),))
    cache_kv = draw_cache_kv(jax.random.fold_in(key_list[9], 71), 0)
    cache_len = draw_cache_len(jax.random.fold_in(key_list[9], 71), 0)
    w_out = centred(key_list[5], (HEADS * HEAD_SIZE, D), (HEADS * HEAD_SIZE // 4) ** -0.5, 0.1875, ((0, 8),))
    gain_mlp = jnp.clip(1.0 + 0.18 * jax.random.normal(key_list[6], (D,), jnp.float32), 0.1, 1.9)
    w_gate_up = centred(key_list[7], (D, 2, FF), D ** -0.5, 0.09375, ((0, 4), (2, 8)))
    w_down = centred(key_list[8], (FF, D), FF ** -0.5, 0.0546875, ((0, 8), (1, 4)))
    return dict(hidden_in=hidden_in, gain_attn=gain_attn, w_qkv=w_qkv, cache_kv=cache_kv, cache_len=cache_len, w_out=w_out, gain_mlp=gain_mlp, w_gate_up=w_gate_up, w_down=w_down)


EPSILON = 1e-05
MASKED = -1e+30

def rms_scale(values_in, gain_vector):
    widened = values_in.astype(jnp.float32)
    mean_square = lax.optimization_barrier(jnp.mean(widened * widened, axis=-1, keepdims=True))
    return (widened * lax.rsqrt(mean_square + EPSILON) * gain_vector.astype(jnp.float32)).astype(jnp.bfloat16)

def reference(hidden_in, gain_attn, w_qkv, cache_kv, cache_len, w_out, gain_mlp, w_gate_up, w_down):
    normed = rms_scale(hidden_in, gain_attn)
    flat_qkv = w_qkv.reshape(D, HEADS * 3 * HEAD_SIZE)
    packed = jnp.dot(normed, flat_qkv, preferred_element_type=jnp.float32).astype(jnp.bfloat16)
    packed = packed.reshape(BATCH, SPAN, HEADS, 3 * HEAD_SIZE).transpose(2, 0, 1, 3)
    cache_heads = cache_kv.transpose(2, 0, 1, 3)
    positions = jnp.arange(CACHE, dtype=jnp.int32)
    valid_cache = positions[None, :] < cache_len.astype(jnp.int32)[:, None]
    usable = jnp.concatenate([valid_cache, jnp.ones((BATCH, SPAN), dtype=bool)], axis=1)

    def one_head(pair):
        head_packed, head_cache = pair
        query_rows = head_packed[:, :, :HEAD_SIZE].astype(jnp.float32)
        joined_key_rows = jnp.concatenate([head_cache[:, :, :HEAD_SIZE], head_packed[:, :, HEAD_SIZE:2 * HEAD_SIZE]], axis=1).astype(jnp.float32)
        joined_value_rows = jnp.concatenate([head_cache[:, :, HEAD_SIZE:], head_packed[:, :, 2 * HEAD_SIZE:]], axis=1).astype(jnp.float32)
        logit_scores = jnp.einsum('nmz,nvz->nmv', query_rows, joined_key_rows) / math.sqrt(HEAD_SIZE)
        logit_scores = jnp.where(usable[:, None, :], logit_scores, MASKED)
        row_peak = lax.optimization_barrier(jnp.max(logit_scores, axis=2, keepdims=True))
        raw_weights = jnp.where(usable[:, None, :], jnp.exp(logit_scores - row_peak), 0.0)
        mass = lax.optimization_barrier(jnp.sum(raw_weights, axis=2))
        rounded_values = lax.optimization_barrier(raw_weights.astype(jnp.bfloat16))
        summed_output = jnp.einsum('qnu,quf->qnf', rounded_values.astype(jnp.float32), joined_value_rows)
        return (summed_output / mass[:, :, None]).astype(jnp.bfloat16)
    heads_out = lax.map(one_head, (packed, cache_heads))
    attended = heads_out.transpose(1, 2, 0, 3).reshape(TOKENS, HEADS * HEAD_SIZE)
    residual = hidden_in.astype(jnp.float32) + jnp.dot(attended, w_out, preferred_element_type=jnp.float32)
    mlp_in = rms_scale(residual, gain_mlp)
    gate = jnp.dot(mlp_in, w_gate_up[:, 0, :], preferred_element_type=jnp.float32)
    upward = jnp.dot(mlp_in, w_gate_up[:, 1, :], preferred_element_type=jnp.float32)
    activated = (jax.nn.silu(gate) * upward).astype(jnp.bfloat16)
    down_sum = jnp.dot(activated, w_down, preferred_element_type=jnp.float32)
    return (residual + down_sum).astype(jnp.bfloat16)
```

```python
import functools
import math

import jax
import jax.numpy as jnp
from jax import lax
from jax.experimental import pallas as pl
from jax.experimental.pallas import tpu as pltpu
from jax.sharding import PartitionSpec as P


EPSILON = 1e-05
MASKED = -1e30
PARTS = 1


def rms_scale(values_in, gain_vector):
    widened = values_in.astype(jnp.float32)
    mean_square = jnp.mean(widened * widened, axis=-1, keepdims=True)
    return (widened * lax.rsqrt(mean_square + EPSILON) * gain_vector).astype(jnp.bfloat16)


def attention_kernel(seqs, heads, chunk, meta, q_ref, kv_ref, own_k, own_v, out_ref):
    seq, head = pl.program_id(0), pl.program_id(2)
    valid, own = meta[seq], meta[seqs + seq]
    width = q_ref.shape[1]
    rows = q_ref.shape[0]
    to_log2 = math.log2(math.e) / math.sqrt(width)
    query = q_ref[...]

    def step(keys, values, bias, carry):
        peak, mass, total = carry
        scores = lax.dot_general(
            query, keys, (((1,), (1,)), ((), ())), preferred_element_type=jnp.float32
        )
        if bias is not None:
            scores = scores + bias
        peak_new = jnp.maximum(peak, jnp.max(scores, axis=1, keepdims=True))
        weights = jnp.exp2((scores - peak_new) * to_log2)
        fade = jnp.exp2((peak - peak_new) * to_log2)
        mass = mass * fade + jnp.sum(weights, axis=1, keepdims=True)
        total = total * fade + jnp.dot(
            weights.astype(jnp.bfloat16), values, preferred_element_type=jnp.float32
        )
        return peak_new, mass, total

    def full_step(i, carry):
        at = pl.multiple_of(i * chunk, chunk)
        return step(
            kv_ref[0, 0, pl.ds(at, chunk), :width],
            kv_ref[0, 0, pl.ds(at, chunk), width:],
            None,
            carry,
        )

    full = valid // chunk

    def tail_step(_, carry):
        at = pl.multiple_of(full * chunk, chunk)
        place = at + lax.broadcasted_iota(jnp.int32, (1, chunk), 1)
        return step(
            kv_ref[0, 0, pl.ds(at, chunk), :width],
            kv_ref[0, 0, pl.ds(at, chunk), width:],
            jnp.where(place < valid, 0.0, MASKED),
            carry,
        )

    carry = (
        jnp.full((rows, 1), MASKED, jnp.float32),
        jnp.zeros((rows, 1), jnp.float32),
        jnp.zeros((rows, width), jnp.float32),
    )
    carry = lax.fori_loop(0, full, full_step, carry)
    carry = lax.fori_loop(0, jnp.where(valid > full * chunk, 1, 0), tail_step, carry)
    carry = lax.fori_loop(
        0, own, lambda _, c: step(own_k[...], own_v[...], None, c), carry
    )
    peak, mass, total = carry
    some = mass > 0.0
    safe = jnp.where(some, mass, 1.0)
    out_ref[:, pl.ds(pl.multiple_of(head * width, width), width)] = (total / safe).astype(
        jnp.bfloat16
    )
    level = jnp.where(some, peak * to_log2 + jnp.log2(safe), MASKED)
    first = level.astype(jnp.bfloat16).astype(jnp.float32)
    second = (level - first).astype(jnp.bfloat16).astype(jnp.float32)
    third = level - first - second
    lane = lax.broadcasted_iota(jnp.int32, (rows, width), 1)
    before = jnp.where(head == 0, 0.0, out_ref[:, heads * width :].astype(jnp.float32))
    marks = jnp.where(lane == 3 * head, first, before)
    marks = jnp.where(lane == 3 * head + 1, second, marks)
    marks = jnp.where(lane == 3 * head + 2, third, marks)
    out_ref[:, heads * width :] = marks.astype(jnp.bfloat16)


def attend(meta, queries, cache_t, packed, seqs, heads, width):
    rows = queries.shape[0] // seqs
    block = math.gcd(rows, 512)
    blocks = rows // block
    cache_rows = cache_t.shape[2]
    own_rows = packed.shape[0]
    chunk = math.gcd(cache_rows, 1024)
    keys = cache_rows + own_rows
    return pl.pallas_call(
        functools.partial(attention_kernel, seqs, heads, chunk),
        grid_spec=pltpu.PrefetchScalarGridSpec(
            num_scalar_prefetch=1,
            grid=(seqs, blocks, heads),
            in_specs=[
                pl.BlockSpec((block, width), lambda s, b, h, m: (s * blocks + b, h)),
                pl.BlockSpec((1, 1, cache_rows, 2 * width), lambda s, b, h, m: (s, h, 0, 0)),
                pl.BlockSpec((own_rows, width), lambda s, b, h, m: (0, 3 * h + 1)),
                pl.BlockSpec((own_rows, width), lambda s, b, h, m: (0, 3 * h + 2)),
            ],
            out_specs=pl.BlockSpec(
                (block, (heads + 1) * width), lambda s, b, h, m: (s * blocks + b, 0)
            ),
        ),
        out_shape=jax.ShapeDtypeStruct((seqs * rows, (heads + 1) * width), jnp.bfloat16),
        compiler_params=pltpu.CompilerParams(vmem_limit_bytes=44 << 20),
        cost_estimate=pl.CostEstimate(
            flops=8 * seqs * rows * heads * keys * width,
            bytes_accessed=2 * seqs * heads * (2 * keys * width + 2 * rows * width),
            transcendentals=seqs * rows * heads * keys,
        ),
    )(meta, queries, cache_t, packed, packed)


def per_device(
    kv_size, hidden_in, gain_attn, w_qkv, cache_kv, cache_len, w_out, gain_mlp, w_gate_up, w_down
):
    heads = w_qkv.shape[1]
    width = w_qkv.shape[2] // 3
    own_rows = hidden_in.shape[0]
    half_rows = own_rows // PARTS
    seqs, cache_rows = cache_kv.shape[0], cache_kv.shape[1]
    kv_index = lax.axis_index("kv")
    model = hidden_in.shape[1]

    def swap(array, bit):
        return lax.ppermute(array, "kv", [(i, i ^ bit) for i in range(kv_size)])

    bits = [1 << i for i in range(kv_size.bit_length() - 1)][::-1]
    order = [0]
    gate_up_set, down_set = [w_gate_up], [w_down]
    for level, bit in enumerate(bits):
        gate_up_set = gate_up_set + [swap(w, bit) for w in gate_up_set]
        down_set = down_set + [swap(w, bit) for w in down_set]
        order = order + [o ^ bit for o in order]

    inputs = [hidden_in[p * half_rows : (p + 1) * half_rows] for p in range(PARTS)]
    flat_qkv = w_qkv.reshape(model, heads * 3 * width)
    cache_t = cache_kv.transpose(0, 2, 1, 3)
    packed_parts, query_parts = [], []
    for part in inputs:
        block_input = lax.all_gather(part, "tp", axis=0, tiled=True)
        normed = rms_scale(block_input, gain_attn)
        packed = jnp.dot(normed, flat_qkv, preferred_element_type=jnp.float32)
        packed = packed.astype(jnp.bfloat16)
        packed_parts.append(packed)
        query_mine = jnp.concatenate(
            [packed[:, 3 * h * width : (3 * h + 1) * width] for h in range(heads)], axis=1
        )
        query_parts.append(lax.all_gather(query_mine, "kv", axis=0, tiled=True))
    packed_all = jnp.concatenate(packed_parts, axis=0)

    valid = jnp.clip(cache_len - kv_index * cache_rows, 0, cache_rows)
    own_seq = kv_index * seqs // kv_size
    own = (jnp.arange(seqs, dtype=jnp.int32) == own_seq).astype(jnp.int32)
    meta = jnp.concatenate([valid.astype(jnp.int32), own])

    residuals, mlp_parts = [], []
    for part, queries in zip(inputs, query_parts):
        partial = attend(meta, queries, cache_t, packed_all, seqs, heads, width)
        partial = partial.reshape(kv_size, queries.shape[0] // kv_size, (heads + 1) * width)
        parts = lax.all_to_all(partial, "kv", split_axis=0, concat_axis=0, tiled=True)
        marks = parts[:, :, heads * width : heads * width + 3 * heads].astype(jnp.float32)
        level = marks.reshape(kv_size, -1, heads, 3).sum(axis=3)
        scaling = jnp.exp2(level - jnp.max(level, axis=0, keepdims=True))
        scaling = scaling / jnp.sum(scaling, axis=0, keepdims=True)
        attended = jnp.concatenate(
            [
                jnp.sum(
                    parts[:, :, h * width : (h + 1) * width].astype(jnp.float32)
                    * scaling[:, :, h : h + 1],
                    axis=0,
                )
                for h in range(heads)
            ],
            axis=1,
        ).astype(jnp.bfloat16)
        terms = jnp.dot(attended, w_out, preferred_element_type=jnp.float32)
        terms = terms.astype(jnp.bfloat16)
        heads_sum = lax.psum_scatter(terms, "tp", scatter_dimension=0, tiled=True)
        residual = part.astype(jnp.float32) + heads_sum.astype(jnp.float32)
        residuals.append(residual)
        mlp_parts.append(
            lax.all_gather(rms_scale(residual, gain_mlp), "tp", axis=0, tiled=True)
        )

    depth = model // kv_size
    outs = []
    for residual, mlp_in in zip(residuals, mlp_parts):
        gate_up = 0.0
        for code, w in zip(order, gate_up_set):
            piece = lax.dynamic_slice_in_dim(mlp_in, (kv_index ^ code) * depth, depth, 1)
            gate_up = gate_up + jnp.einsum(
                "td,dgf->tgf", piece, w, preferred_element_type=jnp.float32
            )
        activated = (jax.nn.silu(gate_up[:, 0, :]) * gate_up[:, 1, :]).astype(jnp.bfloat16)
        terms = jnp.concatenate(
            [
                jnp.dot(activated, w, preferred_element_type=jnp.float32).astype(jnp.bfloat16)
                for w in down_set
            ],
            axis=1,
        )
        down_own = lax.psum_scatter(terms, "tp", scatter_dimension=0, tiled=True)
        blocks = [down_own[:, i * depth : (i + 1) * depth] for i in range(kv_size)]
        for level, bit in enumerate(bits[::-1]):
            flip = (kv_index & bit) != 0
            stride = kv_size >> (level + 1)
            blocks = [jnp.where(flip, blocks[i ^ stride], blocks[i]) for i in range(kv_size)]
        in_place = [None] * kv_size
        for position, code in enumerate(order):
            in_place[code] = blocks[position]
        outs.append(residual + jnp.concatenate(in_place, axis=1).astype(jnp.float32))
    return jnp.concatenate(outs, axis=0).astype(jnp.bfloat16)


def solution(mesh):
    in_specs = (
        P(("kv", "tp"), None),
        P(),
        P(None, "tp", None),
        P(None, "kv", "tp", None),
        P(),
        P("tp", None),
        P(),
        P("kv", None, "tp"),
        P("tp", "kv"),
    )
    out_specs = P(("kv", "tp"), None)
    body = functools.partial(per_device, mesh.shape["kv"])

    return jax.shard_map(body, mesh=mesh, in_specs=in_specs, out_specs=out_specs, check_vma=False)
```
